256 devices in a mesh: dp: 128 (over y, x_lo, z, core), rep: 2 (over x_hi).
Axes of the slice: x: 4 (x_hi: 2, x_lo: 2; x = x_hi * 2 + x_lo), y: 4, z: 8, core: 2. Of those that a mesh axis runs over, the one named last changes fastest.
Arguments:
- q_hidden: bfloat16 [2, 128, 128, 768], P('rep', 'dp'), may hold values from -8 to 8
- p_hidden: bfloat16 [2, 128, 128, 768], P('rep', 'dp'), may hold values from -8 to 8
- w_up: bfloat16 [1536, 768], replicated, may hold values from -0.21875 to 0.21875
- w_down: bfloat16 [1536, 768], replicated, may hold values from -0.15625 to 0.15625
- pos_index: int32 [2, 128], P('rep', 'dp'), may hold values from 0 to 127
- hard_index: int32 [2, 128, 2], P('rep', 'dp'), may hold values from 0 to 127
Outputs:
- w_up_grad: float32 [1536, 768], P(('dp', 'rep'))
- mean_loss: float32 [], replicated
The draws below stay inside these ranges and needn't reach their ends.
All inputs are finite; a program needn't handle non-finite values.
Results may differ from the reference program's by a relative error of at most 0.008.
Values may be sent and summed in bfloat16 or wider, within the bound.
A program may use at most 64 MiB of HBM per device.

```python
import math
import jax
import jax.numpy as jnp
from jax import lax

D = 768
FF = 1536
LEN = 128
HARD = 2
REPLICAS = 2
GQ = 128
GP = 128


def hidden_pair(key):
    shape = (2, REPLICAS, GQ, LEN, D)
    topic = jax.random.normal(jax.random.fold_in(key, 101), (2, REPLICAS, GQ, 1, D), jnp.float32)
    noise = jax.random.normal(jax.random.fold_in(key, 202), shape, jnp.float32)
    both = 0.35 * topic + noise
    return jnp.clip(both, -8.0, 8.0)


def draw_q_hidden(key, part):
    return hidden_pair(key)[0].astype(jnp.bfloat16)


def draw_p_hidden(key, part):
    return hidden_pair(key)[1].astype(jnp.bfloat16)


def place_ends(array, stream_key, low, top_value):
    dims = array.shape
    spot = [jax.random.randint(jax.random.fold_in(stream_key, axis), (), 0, dims[axis]) for axis in range(len(dims))]
    array = array.at[tuple(spot)].set(low)
    longest = dims.index(max(dims))
    spot[longest] = (spot[longest] + 1) % dims[longest]
    return array.at[tuple(spot)].set(top_value)


def normal_values(rng, shape, width, reach, kind=jnp.bfloat16):
    return jnp.clip(width * jax.random.normal(rng, shape, jnp.float32), -reach, reach).astype(kind)


def setup_inputs(seed: int = 0) -> dict:
    keys = jax.random.split(jax.random.key(seed), 7)
    return {
        "q_hidden": draw_q_hidden(jax.random.fold_in(keys[6], 71), 0),
        "p_hidden": draw_p_hidden(jax.random.fold_in(keys[6], 71), 0),
        "w_up": normal_values(keys[2], (FF, D), D ** -0.5, 0.21875),
        "w_down": normal_values(keys[3], (FF, D), FF ** -0.5, 0.15625),
        "pos_index": place_ends(jax.random.randint(keys[4], (REPLICAS, GQ), 0, GP), jax.random.fold_in(keys[4], 1), 0, GP - 1).astype(jnp.int32),
        "hard_index": place_ends(jax.random.randint(keys[5], (REPLICAS, GQ, HARD), 0, GP), jax.random.fold_in(keys[5], 1), 0, GP - 1).astype(jnp.int32),
    }


norm_eps = 1e-06
HARD_BOOST = 1.5

def gelu_slope(values):
    cdf_part = 0.5 * (1.0 + lax.erf(values * (1.0 / math.sqrt(2.0))))
    return cdf_part + values * jnp.exp(-0.5 * values * values) * (1.0 / math.sqrt(2.0 * math.pi))

def encode(seq_block, w_up, w_down):
    tokens = seq_block.reshape(-1, seq_block.shape[-1])
    pre_act = jnp.dot(tokens, w_up.T, preferred_element_type=jnp.float32)
    hidden = jax.nn.gelu(pre_act, approximate=False).astype(jnp.bfloat16)
    summed = tokens.astype(jnp.float32) + jnp.dot(hidden, w_down, preferred_element_type=jnp.float32)
    row_mean = lax.optimization_barrier(jnp.mean(summed, -1, keepdims=True))
    centred = summed - row_mean
    inv_scale = lax.rsqrt(lax.optimization_barrier(jnp.mean(centred * centred, -1, keepdims=True)) + norm_eps)
    normed = centred * inv_scale
    return (tokens, pre_act, hidden, normed, inv_scale)

def backward(pre_act, normed, inv_scale, d_embed, length, w_down):
    grad_out = jnp.repeat(d_embed / length, length, axis=0)
    grad_resid = inv_scale * (grad_out - lax.optimization_barrier(jnp.mean(grad_out, -1, keepdims=True)) - normed * lax.optimization_barrier(jnp.mean(grad_out * normed, -1, keepdims=True)))
    grad_low = grad_resid.astype(jnp.bfloat16)
    grad_hidden = jnp.dot(grad_low, w_down.T, preferred_element_type=jnp.float32)
    grad_pre = (grad_hidden * gelu_slope(pre_act)).astype(jnp.bfloat16)
    return (grad_low, grad_pre)

def reference(q_hidden, p_hidden, w_up, w_down, pos_index, hard_index):
    block_rows = 8
    every_seq = jnp.concatenate([q_hidden.reshape(-1, LEN, D), p_hidden.reshape(-1, LEN, D)], 0)
    blocks = every_seq.reshape(-1, block_rows, LEN, D)

    def embed(seq_block):
        normed = encode(seq_block, w_up, w_down)[3]
        return lax.optimization_barrier(jnp.mean(normed.reshape(block_rows, LEN, D), 1)).astype(jnp.bfloat16)
    embedded = lax.map(embed, blocks).reshape(2, REPLICAS, GQ, D)
    query_embed = embedded[0]
    passage_embed = embedded[1]
    scores = jnp.einsum('rqd,rpd->rqp', query_embed.astype(jnp.float32), passage_embed.astype(jnp.float32))
    columns = jnp.arange(GP, dtype=jnp.int32)
    hard_mask = jnp.any(hard_index[..., None] == columns, axis=-2)
    logits = scores + HARD_BOOST * hard_mask.astype(jnp.float32)
    row_max = lax.optimization_barrier(jnp.max(logits, -1, keepdims=True))
    log_total = row_max + jnp.log(lax.optimization_barrier(jnp.sum(jnp.exp(logits - row_max), -1, keepdims=True)))
    target = pos_index[..., None] == columns
    picked = lax.optimization_barrier(jnp.sum(jnp.where(target, logits, 0.0), -1))
    loss_sum = jnp.sum(log_total[..., 0] - picked)
    weights = (jnp.exp(logits - log_total) - target.astype(jnp.float32)).astype(jnp.bfloat16)
    d_query = jnp.einsum('rqp,rpd->rqd', weights.astype(jnp.float32), passage_embed.astype(jnp.float32))
    d_passage = jnp.einsum('rqp,rqd->rpd', weights.astype(jnp.float32), query_embed.astype(jnp.float32))
    d_all = jnp.concatenate([d_query.reshape(-1, D), d_passage.reshape(-1, D)], 0).reshape(-1, block_rows, D)

    def accumulate(up_sum, items):
        seq_block, d_embed = items
        tokens, pre_act, hidden, normed, inv_scale = encode(seq_block, w_up, w_down)
        grad_low, grad_pre = backward(pre_act, normed, inv_scale, d_embed, LEN, w_down)
        up_sum = up_sum + jnp.dot(grad_pre.T, tokens, preferred_element_type=jnp.float32)
        return (up_sum, None)
    up_sum, unused = lax.scan(accumulate, jnp.zeros((FF, D), jnp.float32), (blocks, d_all))
    return (up_sum, loss_sum / (REPLICAS * GQ))
```

```python
import math

import jax
import jax.numpy as jnp
from jax import lax
from jax.experimental import pallas as pl
from jax.experimental.pallas import tpu as pltpu
from jax.sharding import PartitionSpec as P

MESH = pl.DeviceIdType.MESH
BF16 = jnp.bfloat16
F32 = jnp.float32

NX, NY, NZ = 4, 4, 8
D, FF, LEN = 768, 1536, 128
GROUP = 128
NORM_EPS = 1e-06
HARD_BOOST = 1.5
CHUNKS = 6
CH = FF // CHUNKS
YB = FF // NY
XB = YB // 2 // NX
HALF = D // 2
OWN = XB // NZ


def nt(left, right):
    return lax.dot_general(left, right, (((1,), (1,)), ((), ())), preferred_element_type=F32)


def nn(left, right):
    return lax.dot_general(left, right, (((1,), (0,)), ((), ())), preferred_element_type=F32)


def cdf(v):
    return 0.5 * (1.0 + lax.erf(v * (1.0 / math.sqrt(2.0))))


def iota(shape, dim):
    return lax.broadcasted_iota(jnp.int32, shape, dim)


def kernel(
    pos_ref, hard_ref, q_hbm, p_hbm, wup_hbm, wdn_hbm,
    out_ref, loss_ref,
    x_v, wup_v, wdn_v, wupp_v, wdnp_v, hid_v, normed_v, scale_v, slope_v, gr_v,
    gb, gf, qall, pall,
    ts, cr, tf, ra, rb, oa, ob, rcv_a, rcv_b, sec_a, sec_b, s2a, s2b, r2a, r2b, zs, zr, lsend, lrecv,
    sem_in, z_s, z_r, g_s, g_r, c_s, c_r, l_s, l_r, core_s, core_r, a_s, a_r, b_s, b_r, x2_s, x2_r, y2_s, y2_r, zz_s, zz_r,
):
    dp = lax.axis_index("dp")
    xh = lax.axis_index("rep")
    core = lax.rem(dp, 2)
    z = lax.rem(lax.div(dp, 2), NZ)
    xl = lax.rem(lax.div(dp, 2 * NZ), 2)
    y = lax.div(dp, 4 * NZ)
    x = xh * 2 + xl

    def device(y_, x_, z_, core_):
        return (((y_ * 2 + lax.rem(x_, 2)) * NZ + z_) * 2 + core_, lax.div(x_, 2))

    def ymod(k):
        return lax.rem(y + k, NY)

    def xmod(k):
        return lax.rem(x + k, NX)

    def zmod(k):
        return lax.rem(z + k, NZ)

    partner = device(y, x, z, 1 - core)

    def plane(dy, dxl):
        xl_ = lax.rem(xl + dxl, 2)
        return ymod(dy), xl_, device(ymod(dy), xh * 2 + xl_, z, core)

    loads = []

    def load(src, dst):
        copy = pltpu.make_async_copy(src, dst, sem_in.at[len(loads)])
        copy.start()
        loads.append(copy)
        return copy

    x_loads = [load(q_hbm, x_v.at[0:LEN]), load(p_hbm, x_v.at[LEN : 2 * LEN])]
    up_loads = [load(wup_hbm.at[c * CH : (c + 1) * CH], wup_v.at[c * CH : (c + 1) * CH]) for c in range(CHUNKS)]
    dn_loads = [load(wdn_hbm.at[c * CH : (c + 1) * CH], wdn_v.at[c * CH : (c + 1) * CH]) for c in range(CHUNKS)]

    barrier = pltpu.get_barrier_semaphore()
    peers = [partner]
    peers += [device(y, x, zmod(k), core) for k in range(1, NZ)]
    peers += [plane(dy, dxl)[2] for dy in range(NY) for dxl in range(2) if dy or dxl]
    peers += [device(y, xmod(k), z, core) for k in range(1, NX)]
    for peer in peers:
        pl.semaphore_signal(barrier, inc=1, device_id=peer, device_id_type=MESH)

    for copy in x_loads:
        copy.wait()
    tokens = x_v[...]
    for c in range(CHUNKS):
        up_loads[c].wait()
        pre = nt(tokens, wup_v[c * CH : (c + 1) * CH, :])
        hid_v[:, c * CH : (c + 1) * CH] = (pre * cdf(pre)).astype(BF16)
    for copy in dn_loads:
        copy.wait()
    summed = tokens.astype(F32) + nn(hid_v[...], wdn_v[...])
    centred = summed - jnp.mean(summed, -1, keepdims=True)
    inv_scale = lax.rsqrt(jnp.mean(centred * centred, -1, keepdims=True) + NORM_EPS)
    normed = centred * inv_scale
    normed_v[...] = normed
    scale_v[...] = jnp.broadcast_to(inv_scale, (2 * LEN, 128))
    embed_q = jnp.sum(normed[:LEN], 0, keepdims=True) * (1.0 / LEN)
    embed_p = jnp.sum(normed[LEN:], 0, keepdims=True) * (1.0 / LEN)

    row = iota((16, 128), 0)
    lane = iota((16, 128), 1)
    tile = jnp.zeros((16, 128), F32)
    for k in range(6):
        tile = jnp.where(row == k, embed_q[:, k * 128 : (k + 1) * 128], tile)
        tile = jnp.where(row == 6 + k, embed_p[:, k * 128 : (k + 1) * 128], tile)
    named = jnp.where(lane == 0, pos_ref[0, 0], jnp.where(lane == 1, hard_ref[0, 0], hard_ref[0, 1]))
    tile = jnp.where(row == 12, named.astype(F32), tile)
    gb[y, xl, core, z] = tile.astype(BF16)

    pl.semaphore_wait(barrier, len(peers))

    def remote(src, dst, send, recv, to):
        return pltpu.make_async_remote_copy(
            src_ref=src, dst_ref=dst, send_sem=send, recv_sem=recv, device_id=to, device_id_type=MESH
        )

    sends = []
    own_tile = gb.at[y, xl, core, z]
    for k in range(1, NZ):
        copy = remote(own_tile, own_tile, z_s.at[k], z_r.at[k], device(y, x, zmod(k), core))
        copy.start()
        sends.append(copy)

    out_row = iota((YB, YB), 0)
    in_row = iota((YB, YB), 1)
    unit = lax.shift_right_logical(out_row * 10923, 16)
    inner = out_row - unit * 6
    slot_z = jnp.bitwise_and(unit, 7)
    slot_x = jnp.bitwise_and(lax.shift_right_logical(unit, 3), 3)
    slot_c = lax.shift_right_logical(unit, 5)
    to_z = jnp.bitwise_and(slot_z + z, 7)
    to_x = jnp.bitwise_and(slot_x + x, 3)
    to_c = jnp.where(slot_c == 0, 1 - core, core)
    to_xh = lax.shift_right_logical(to_x, 1)
    to_xl = jnp.bitwise_and(to_x, 1)
    source = (((to_xl * NZ + to_z) * 2 + to_c) * 2 + to_xh) * 6 + inner
    reorder = (source == in_row).astype(F32).astype(BF16)
    for sy in range(NY):
        rows = pl.ds(pl.multiple_of(ymod(sy) * YB, YB), YB)
        wdnp_v[sy] = nn(reorder, wdn_v[rows, :]).astype(BF16)

    for k in range(1, NZ):
        landed = gb.at[y, xl, core, zmod(NZ - k)]
        remote(landed, landed, z_s.at[k], z_r.at[k], device(y, x, zmod(k), core)).wait_recv()
    own_line = gb.at[y, xl, core]
    copy = remote(own_line, own_line, c_s.at[0], c_r.at[0], partner)
    copy.start()
    sends.append(copy)
    offsets = [(0, 1), (1, 0), (3, 0), (1, 1), (3, 1), (2, 0), (2, 1)]
    for dy, dxl in offsets:
        copy = remote(own_line, own_line, g_s.at[dy * 2 + dxl], g_r.at[dy * 2 + dxl], plane(dy, dxl)[2])
        copy.start()
        sends.append(copy)

    for sy in range(NY):
        rows = pl.ds(pl.multiple_of(ymod(sy) * YB, YB), YB)
        wupp_v[sy] = nn(reorder, wup_v[rows, :]).astype(BF16)
        pre = nt(wupp_v[sy], tokens)
        slope_v[sy] = cdf(pre) + pre * jnp.exp(-0.5 * pre * pre) * (1.0 / math.sqrt(2.0 * math.pi))

    for dy, dxl in offsets:
        y_, xl_, _ = plane(NY - dy, dxl)
        landed = gb.at[y_, xl_, core]
        remote(landed, landed, g_s.at[dy * 2 + dxl], g_r.at[dy * 2 + dxl], partner).wait_recv()
        copy = remote(landed, landed, c_s.at[dy * 2 + dxl], c_r.at[dy * 2 + dxl], partner)
        copy.start()
        sends.append(copy)
    for dy, dxl in [(0, 0)] + offsets:
        y_, xl_, _ = plane(NY - dy, dxl)
        landed = gb.at[y_, xl_, 1 - core]
        remote(landed, landed, c_s.at[dy * 2 + dxl], c_r.at[dy * 2 + dxl], partner).wait_recv()

    gf[...] = gb[...].reshape(GROUP * 16, 128).astype(F32)
    for k in range(6):
        qall[:, k * 128 : (k + 1) * 128] = gf[pl.ds(k, GROUP, stride=16), :].astype(BF16)
        pall[:, k * 128 : (k + 1) * 128] = gf[pl.ds(6 + k, GROUP, stride=16), :].astype(BF16)
    names = gf[pl.ds(12, GROUP, stride=16), :]
    scores = nt(qall[...], pall[...])
    place = iota((GROUP, GROUP), 1)
    group_index = (
        lax.shift_right_logical(place, 4) * 16
        + jnp.bitwise_and(place, 7) * 2
        + jnp.bitwise_and(lax.shift_right_logical(place, 3), 1)
    ).astype(F32)
    target = names[:, 0:1] == group_index
    hard = (names[:, 1:2] == group_index) | (names[:, 2:3] == group_index)
    logits = scores + jnp.where(hard, HARD_BOOST, 0.0)
    row_max = jnp.max(logits, -1, keepdims=True)
    log_total = row_max + jnp.log(jnp.sum(jnp.exp(logits - row_max), -1, keepdims=True))
    picked = jnp.sum(jnp.where(target, logits, 0.0), -1, keepdims=True)
    loss_sum = jnp.sum(log_total - picked, 0, keepdims=True)
    lsend[...] = jnp.broadcast_to(loss_sum, (8, 128))
    weights = (jnp.exp(logits - log_total) - jnp.where(target, 1.0, 0.0)).astype(BF16)
    mine = ((y * 2 + xl) * 2 + core) * NZ + z
    pick = (iota((16, GROUP), 1) == mine).astype(F32).astype(BF16)
    own_row = nn(pick, weights).astype(BF16)
    own_col = nt(pick, weights).astype(BF16)
    grad_q = nn(own_row, pall[...])[0:1] * (1.0 / LEN)
    grad_p = nn(own_col, qall[...])[0:1] * (1.0 / LEN)

    other = device(y, xmod(2), z, core)
    loss_copy = remote(lsend, lrecv, l_s.at[0], l_r.at[0], other)
    loss_copy.start()
    sends.append(loss_copy)

    for part, grad in ((0, grad_q), (1, grad_p)):
        rows = slice(part * LEN, (part + 1) * LEN)
        normed = normed_v[rows, :]
        along = jnp.mean(normed * grad, -1, keepdims=True)
        resid = grad - jnp.mean(grad, -1, keepdims=True) - normed * along
        gr_v[rows, :] = (scale_v[rows, 0:1] * resid).astype(BF16)
    resid = gr_v[...]
    order = (2, 1, 3, 0)
    core_copies = {}
    for sy in order:
        grad_pre = (nt(wdnp_v[sy], resid) * slope_v[sy]).astype(BF16)
        terms = nn(grad_pre, tokens)
        ts[sy] = terms[: YB // 2].reshape(NX, XB, D).astype(BF16)
        tf[sy] = terms[YB // 2 :].reshape(NX, XB, D)
        copy = remote(ts.at[sy], cr.at[sy], core_s.at[sy], core_r.at[sy], partner)
        copy.start()
        core_copies[sy] = copy
        sends.append(copy)

    y_up, y_dn = device(ymod(1), x, z, core), device(ymod(3), x, z, core)
    x_up, x_dn = device(y, xmod(1), z, core), device(y, xmod(3), z, core)
    colours = {"a": (ra, rcv_a, a_s, a_r, y_up, y_dn), "b": (rb, rcv_b, b_s, b_r, x_up, x_dn)}
    ring = {}

    def ring_send(colour, index, src):
        _, rcv, send, recv, up, down = colours[colour]
        to = up if index in (0, 1, 4) else down
        copy = remote(src, rcv.at[index], send.at[index], recv.at[index], to)
        copy.start()
        sends.append(copy)
        ring[colour, index] = copy

    for sy in order:
        core_copies[sy].wait_recv()
        got = tf[sy] + cr[sy].astype(F32)
        if sy == 0:
            oa[...] = got[:, :, :HALF]
        else:
            ra[sy] = got[:, :, :HALF].astype(BF16)
        ob[sy] = got[0, :, HALF:]
        for sx in range(1, NX):
            rb[sx, sy] = got[sx, :, HALF:].astype(BF16)
        if sy == 2:
            ring_send("a", 0, ra.at[2, 0:2])
            ring_send("a", 2, ra.at[2, 2:4])
        elif sy == 1:
            ring_send("a", 1, ra.at[1, 2:4])
        elif sy == 3:
            ring_send("a", 3, ra.at[3, 0:2])
            ring_send("b", 2, rb.at[2, 2:4])
            ring_send("b", 1, rb.at[1, 2:4])
        else:
            ring_send("b", 0, rb.at[2, 0:2])
            ring_send("b", 3, rb.at[3, 0:2])

    for colour, mid, sec in (("a", ra, sec_a), ("b", rb, sec_b)):
        rcv = colours[colour][1]
        ring[colour, 0].wait_recv()
        sec[0] = (mid[1, 0:2].astype(F32) + rcv[0].astype(F32)).astype(BF16)
        ring_send(colour, 4, sec.at[0])
        ring[colour, 2].wait_recv()
        sec[1] = (mid[3, 2:4].astype(F32) + rcv[2].astype(F32)).astype(BF16)
        ring_send(colour, 5, sec.at[1])

    second = {}
    for colour, own, s2, r2, send, recv in (("a", oa, s2a, r2a, x2_s, x2_r), ("b", ob, s2b, r2b, y2_s, y2_r)):
        rcv = colours[colour][1]
        ring[colour, 1].wait_recv()
        ring[colour, 3].wait_recv()
        ring[colour, 4].wait_recv()
        ring[colour, 5].wait_recv()
        own[0:2] = own[0:2] + rcv[3].astype(F32) + rcv[4].astype(F32)
        own[2:4] = own[2:4] + rcv[1].astype(F32) + rcv[5].astype(F32)
        for k in (2, 1, 3):
            s2[k] = own[k].astype(BF16)
            to = device(y, xmod(k), z, core) if colour == "a" else device(ymod(k), x, z, core)
            copy = remote(s2.at[k], r2.at[k], send.at[k], recv.at[k], to)
            copy.start()
            sends.append(copy)
            second[colour, k] = copy

    sums = []
    for colour, own, r2 in (("a", oa, r2a), ("b", ob, r2b)):
        total = own[0]
        for k in (1, 3, 2):
            second[colour, k].wait_recv()
            total = total + r2[k].astype(F32)
        sums.append(total)
    total = jnp.concatenate(sums, -1)

    spread_row = iota((NZ * 8, XB), 0)
    spread_of = lax.shift_right_logical(spread_row, 3) * OWN + jnp.bitwise_and(spread_row, 7)
    spread = (spread_of == iota((NZ * 8, XB), 1)) & (jnp.bitwise_and(spread_row, 7) < OWN)
    zs[...] = nn(spread.astype(F32).astype(BF16), total.astype(BF16)).reshape(NZ, 8, D).astype(BF16)
    last = []
    for k in (4, 3, 5, 2, 6, 1, 7):
        copy = remote(zs.at[k], zr.at[k], zz_s.at[k], zz_r.at[k], device(y, x, zmod(k), core))
        copy.start()
        sends.append(copy)
        last.append((k, copy))
    loss_copy.wait_recv()
    loss_ref[...] = (lsend[0:1, 0:1] + lrecv[0:1, 0:1]) * (1.0 / (2 * GROUP))
    final = total[0:OWN]
    for k, copy in reversed(last):
        copy.wait_recv()
        final = final + zr[k].astype(F32)[0:OWN]
    out_ref[...] = final
    for copy in sends:
        copy.wait_send()


def shards(q_hidden, p_hidden, w_up, w_down, pos_index, hard_index):
    vm = pltpu.VMEM
    dma = pltpu.SemaphoreType.DMA
    scratch = [
        vm((2 * LEN, D), BF16), vm((FF, D), BF16), vm((FF, D), BF16),
        vm((NY, YB, D), BF16), vm((NY, YB, D), BF16), vm((2 * LEN, FF), BF16),
        vm((2 * LEN, D), F32), vm((2 * LEN, 128), F32), vm((NY, YB, 2 * LEN), F32), vm((2 * LEN, D), BF16),
        vm((NY, 2, 2, NZ, 16, 128), BF16), vm((GROUP * 16, 128), F32), vm((GROUP, D), BF16), vm((GROUP, D), BF16),
        vm((NY, NX, XB, D), BF16), vm((NY, NX, XB, D), BF16), vm((NY, NX, XB, D), F32),
        vm((NY, NX, XB, HALF), BF16), vm((NX, NY, XB, HALF), BF16),
        vm((NX, XB, HALF), F32), vm((NY, XB, HALF), F32),
        vm((6, 2, XB, HALF), BF16), vm((6, 2, XB, HALF), BF16),
        vm((2, 2, XB, HALF), BF16), vm((2, 2, XB, HALF), BF16),
        vm((4, XB, HALF), BF16), vm((4, XB, HALF), BF16), vm((4, XB, HALF), BF16), vm((4, XB, HALF), BF16),
        vm((NZ, 8, D), BF16), vm((NZ, 8, D), BF16), vm((8, 128), F32), vm((8, 128), F32),
        dma((2 + 2 * CHUNKS,)), dma((8,)), dma((8,)), dma((8,)), dma((8,)), dma((8,)), dma((8,)), dma((1,)), dma((1,)),
        dma((4,)), dma((4,)), dma((6,)), dma((6,)), dma((6,)), dma((6,)),
        dma((4,)), dma((4,)), dma((4,)), dma((4,)), dma((8,)), dma((8,)),
    ]
    hbm = pl.BlockSpec(memory_space=pl.ANY)
    smem = pl.BlockSpec(memory_space=pltpu.SMEM)
    out, loss = pl.pallas_call(
        kernel,
        out_shape=(jax.ShapeDtypeStruct((OWN, D), F32), jax.ShapeDtypeStruct((1, 1), F32)),
        in_specs=[smem, smem, hbm, hbm, hbm, hbm],
        out_specs=(pl.BlockSpec(memory_space=pltpu.VMEM), pl.BlockSpec(memory_space=pltpu.VMEM)),
        scratch_shapes=scratch,
        compiler_params=pltpu.CompilerParams(
            collective_id=0, has_side_effects=True, vmem_limit_bytes=56 * 1024 * 1024
        ),
    )(pos_index, hard_index[0], q_hidden[0, 0], p_hidden[0, 0], w_up, w_down)
    return out, loss[0, 0]


def solution(mesh):
    return jax.shard_map(
        shards,
        mesh=mesh,
        in_specs=(
            P("rep", "dp", None, None),
            P("rep", "dp", None, None),
            P(),
            P(),
            P("rep", "dp"),
            P("rep", "dp", None),
        ),
        out_specs=(P(("dp", "rep"), None), P()),
        check_vma=False,
    )
```

```python
import math

import jax
import jax.numpy as jnp
from jax import lax
from jax.experimental import pallas as pl
from jax.experimental.pallas import tpu as pltpu
from jax.sharding import PartitionSpec as P

MESH = pl.DeviceIdType.MESH
BF16 = jnp.bfloat16
F32 = jnp.float32

NX, NY, NZ = 4, 4, 8
D, FF, LEN = 768, 1536, 128
GROUP = 128
NORM_EPS = 1e-06
HARD_BOOST = 1.5
CHUNKS = 6
CH = FF // CHUNKS
YB = FF // NY
CB = YB // 2
XB = CB // NX
ORDER = (2, 3, 1, 0)
HALF = D // 2
OWN = XB // NZ
VMEM_LIMIT = 56 * 1024 * 1024


def nt(left, right):
    return lax.dot_general(left, right, (((1,), (1,)), ((), ())), preferred_element_type=F32)


def nn(left, right):
    return lax.dot_general(left, right, (((1,), (0,)), ((), ())), preferred_element_type=F32)


def cdf(v):
    return 0.5 * (1.0 + lax.erf(v * (1.0 / math.sqrt(2.0))))


def iota(shape, dim):
    return lax.broadcasted_iota(jnp.int32, shape, dim)


def kernel(
    pos_hbm, hard_hbm, q_hbm, p_hbm, wup_hbm, wdn_hbm,
    out_ref, loss_ref,
    pos_ref, hard_ref, x_v, wup_v, wdn_v, wupp_v, wdnp_v, hid_v, normed_v, scale_v, slope_v, gr_v,
    gb, gf, qall, pall,
    ra, rb, oa, ob, rcv_a, rcv_b, sec_a, sec_b, s2a, s2b, r2a, r2b, zs, zr, lsend, lrecv,
    sem_in, z_s, z_r, g_s, g_r, c_s, c_r, l_s, l_r, core_s, core_r, a_s, a_r, b_s, b_r, x2_s, x2_r, y2_s, y2_r, zz_s, zz_r,
):
    dp = lax.axis_index("dp")
    xh = lax.axis_index("rep")
    core = lax.rem(dp, 2)
    z = lax.rem(lax.div(dp, 2), NZ)
    xl = lax.rem(lax.div(dp, 2 * NZ), 2)
    y = lax.div(dp, 4 * NZ)
    x = xh * 2 + xl

    def device(y_, x_, z_, core_):
        return (((y_ * 2 + lax.rem(x_, 2)) * NZ + z_) * 2 + core_, lax.div(x_, 2))

    def ymod(k):
        return lax.rem(y + k, NY)

    def xmod(k):
        return lax.rem(x + k, NX)

    def zmod(k):
        return lax.rem(z + k, NZ)

    partner = device(y, x, z, 1 - core)

    def plane(dy, dxl):
        xl_ = lax.rem(xl + dxl, 2)
        return ymod(dy), xl_, device(ymod(dy), xh * 2 + xl_, z, core)

    loads = []

    def load(src, dst):
        copy = pltpu.make_async_copy(src, dst, sem_in.at[len(loads)])
        copy.start()
        loads.append(copy)
        return copy

    x_loads = [load(q_hbm, x_v.at[0:LEN]), load(p_hbm, x_v.at[LEN : 2 * LEN])]
    up_loads = [load(wup_hbm.at[c * CH : (c + 1) * CH], wup_v.at[c * CH : (c + 1) * CH]) for c in range(CHUNKS)]
    index_loads = [load(pos_hbm, pos_ref), load(hard_hbm, hard_ref)]
    dn_loads = [load(wdn_hbm.at[c * CH : (c + 1) * CH], wdn_v.at[c * CH : (c + 1) * CH]) for c in range(CHUNKS)]

    barrier = pltpu.get_barrier_semaphore()
    peers = [partner]
    peers += [device(y, x, zmod(k), core) for k in range(1, NZ)]
    peers += [plane(dy, dxl)[2] for dy in range(NY) for dxl in range(2) if dy or dxl]
    peers += [device(y, xmod(k), z, core) for k in range(1, NX)]
    for peer in peers:
        pl.semaphore_signal(barrier, inc=1, device_id=peer, device_id_type=MESH)

    for copy in x_loads:
        copy.wait()
    tokens = x_v[: 2 * LEN, :]
    for c in range(CHUNKS):
        up_loads[c].wait()
        pre = nt(tokens, wup_v[c * CH : (c + 1) * CH, :])
        hid_v[:, c * CH : (c + 1) * CH] = (pre * cdf(pre)).astype(BF16)
    for copy in dn_loads:
        copy.wait()
    summed = tokens.astype(F32) + nn(hid_v[...], wdn_v[...])
    centred = summed - jnp.mean(summed, -1, keepdims=True)
    inv_scale = lax.rsqrt(jnp.mean(centred * centred, -1, keepdims=True) + NORM_EPS)
    normed = centred * inv_scale
    normed_v[: 2 * LEN, :] = normed.astype(BF16)
    scale_v[: 2 * LEN, :] = jnp.broadcast_to(inv_scale, (2 * LEN, 128))
    embed_q = jnp.sum(normed[:LEN], 0, keepdims=True) * (1.0 / LEN)
    embed_p = jnp.sum(normed[LEN:], 0, keepdims=True) * (1.0 / LEN)

    for copy in index_loads:
        copy.wait()
    row = iota((16, 128), 0)
    lane = iota((16, 128), 1)
    tile = jnp.zeros((16, 128), F32)
    for k in range(6):
        tile = jnp.where(row == k, embed_q[:, k * 128 : (k + 1) * 128], tile)
        tile = jnp.where(row == 6 + k, embed_p[:, k * 128 : (k + 1) * 128], tile)
    named = jnp.where(lane == 0, pos_ref[0, 0], jnp.where(lane == 1, hard_ref[0, 0], hard_ref[0, 1]))
    tile = jnp.where(row == 12, named.astype(F32), tile)
    gb[y, xl, core, z] = tile.astype(BF16)

    pl.semaphore_wait(barrier, len(peers))

    def remote(src, dst, send, recv, to):
        return pltpu.make_async_remote_copy(
            src_ref=src, dst_ref=dst, send_sem=send, recv_sem=recv, device_id=to, device_id_type=MESH
        )

    sends = []
    own_tile = gb.at[y, xl, core, z]
    for k in range(1, NZ):
        copy = remote(own_tile, own_tile, z_s.at[k], z_r.at[k], device(y, x, zmod(k), core))
        copy.start()
        sends.append(copy)

    shared = []
    for k, buf in enumerate((x_v, normed_v, scale_v)):
        copy = remote(
            buf.at[: 2 * LEN], buf.at[2 * LEN :], core_s.at[k], core_r.at[k], partner
        )
        copy.start()
        shared.append(copy)
        sends.append(copy)

    out_row = iota((CB, YB), 0)
    in_row = iota((CB, YB), 1)
    unit = lax.shift_right_logical(out_row * 10923, 16)
    inner = out_row - unit * 6
    slot_z = jnp.bitwise_and(unit, 7)
    slot_x = lax.shift_right_logical(unit, 3)
    to_z = jnp.bitwise_and(slot_z + z, 7)
    to_x = jnp.bitwise_and(slot_x + x, 3)
    to_xh = lax.shift_right_logical(to_x, 1)
    to_xl = jnp.bitwise_and(to_x, 1)
    source = (((to_xl * NZ + to_z) * 2 + core) * 2 + to_xh) * 6 + inner
    reorder = (source == in_row).astype(F32).astype(BF16)
    for i, sy in enumerate(ORDER):
        rows = pl.ds(pl.multiple_of(ymod(sy) * YB, YB), YB)
        wdnp_v[i * CB : (i + 1) * CB, :] = nn(reorder, wdn_v[rows, :]).astype(BF16)

    for k in range(1, NZ):
        landed = gb.at[y, xl, core, zmod(NZ - k)]
        remote(landed, landed, z_s.at[k], z_r.at[k], device(y, x, zmod(k), core)).wait_recv()
    own_line = gb.at[y, xl, core]
    copy = remote(own_line, own_line, c_s.at[0], c_r.at[0], partner)
    copy.start()
    sends.append(copy)
    offsets = [(0, 1), (1, 0), (3, 0), (1, 1), (3, 1), (2, 0), (2, 1)]
    for dy, dxl in offsets:
        copy = remote(own_line, own_line, g_s.at[dy * 2 + dxl], g_r.at[dy * 2 + dxl], plane(dy, dxl)[2])
        copy.start()
        sends.append(copy)

    for i, sy in enumerate(ORDER):
        rows = pl.ds(pl.multiple_of(ymod(sy) * YB, YB), YB)
        wupp_v[i * CB : (i + 1) * CB, :] = nn(reorder, wup_v[rows, :]).astype(BF16)
    for copy in shared:
        copy.wait_recv()
    both = x_v[...]
    for i in range(2):
        block = slice(i * YB, (i + 1) * YB)
        pre = nt(wupp_v[block, :], both)
        slope_v[block, :] = cdf(pre) + pre * jnp.exp(-0.5 * pre * pre) * (1.0 / math.sqrt(2.0 * math.pi))

    for dy, dxl in offsets:
        y_, xl_, _ = plane(NY - dy, dxl)
        landed = gb.at[y_, xl_, core]
        remote(landed, landed, g_s.at[dy * 2 + dxl], g_r.at[dy * 2 + dxl], partner).wait_recv()
        copy = remote(landed, landed, c_s.at[dy * 2 + dxl], c_r.at[dy * 2 + dxl], partner)
        copy.start()
        sends.append(copy)
    for dy, dxl in [(0, 0)] + offsets:
        y_, xl_, _ = plane(NY - dy, dxl)
        landed = gb.at[y_, xl_, 1 - core]
        remote(landed, landed, c_s.at[dy * 2 + dxl], c_r.at[dy * 2 + dxl], partner).wait_recv()

    gf[...] = gb[...].reshape(GROUP * 16, 128).astype(F32)
    for k in range(6):
        qall[:, k * 128 : (k + 1) * 128] = gf[pl.ds(k, GROUP, stride=16), :].astype(BF16)
        pall[:, k * 128 : (k + 1) * 128] = gf[pl.ds(6 + k, GROUP, stride=16), :].astype(BF16)
    names = gf[pl.ds(12, GROUP, stride=16), :]
    scores = nt(qall[...], pall[...])
    place = iota((GROUP, GROUP), 1)
    group_index = (
        lax.shift_right_logical(place, 4) * 16
        + jnp.bitwise_and(place, 7) * 2
        + jnp.bitwise_and(lax.shift_right_logical(place, 3), 1)
    ).astype(F32)
    target = names[:, 0:1] == group_index
    hard = (names[:, 1:2] == group_index) | (names[:, 2:3] == group_index)
    logits = scores + jnp.where(hard, HARD_BOOST, 0.0)
    row_max = jnp.max(logits, -1, keepdims=True)
    log_total = row_max + jnp.log(jnp.sum(jnp.exp(logits - row_max), -1, keepdims=True))
    picked = jnp.sum(jnp.where(target, logits, 0.0), -1, keepdims=True)
    loss_sum = jnp.sum(log_total - picked, 0, keepdims=True)
    lsend[...] = jnp.broadcast_to(loss_sum, (8, 128))
    weights = (jnp.exp(logits - log_total) - jnp.where(target, 1.0, 0.0)).astype(BF16)
    mine = (y * 2 + xl) * 2 * NZ + z
    pick_core = jnp.where(iota((16, GROUP), 0) < 8, core, 1 - core)
    pick = (iota((16, GROUP), 1) == mine + pick_core * NZ).astype(F32).astype(BF16)
    own_row = nn(pick, weights).astype(BF16)
    own_col = nt(pick, weights).astype(BF16)
    grad_q = nn(own_row, pall[...]) * (1.0 / LEN)
    grad_p = nn(own_col, qall[...]) * (1.0 / LEN)

    other = device(y, xmod(2), z, core)
    loss_copy = remote(lsend, lrecv, l_s.at[0], l_r.at[0], other)
    loss_copy.start()
    sends.append(loss_copy)

    for part, grad in enumerate((grad_q[0:1], grad_p[0:1], grad_q[8:9], grad_p[8:9])):
        rows = slice(part * LEN, (part + 1) * LEN)
        normed = normed_v[rows, :].astype(F32)
        offset = grad - jnp.mean(grad, -1, keepdims=True)
        along = jnp.mean(normed * offset, -1, keepdims=True)
        gr_v[rows, :] = (scale_v[rows, 0:1] * (offset - normed * along)).astype(BF16)
    resid = gr_v[...]

    y_up, y_dn = device(ymod(1), x, z, core), device(ymod(3), x, z, core)
    x_up, x_dn = device(y, xmod(1), z, core), device(y, xmod(3), z, core)
    colours = {"a": (ra, rcv_a, a_s, a_r, y_up, y_dn), "b": (rb, rcv_b, b_s, b_r, x_up, x_dn)}
    ring = {}

    def ring_send(colour, index, src):
        _, rcv, send, recv, up, down = colours[colour]
        to = up if index in (0, 1, 4) else down
        copy = remote(src, rcv.at[index], send.at[index], recv.at[index], to)
        copy.start()
        sends.append(copy)
        ring[colour, index] = copy

    for i in range(2):
        block = slice(i * YB, (i + 1) * YB)
        grad_pre = (nt(wdnp_v[block, :], resid) * slope_v[block, :]).astype(BF16)
        pair = nn(grad_pre, both).reshape(2, NX, XB, D)
        for sy, terms in zip(ORDER[2 * i : 2 * i + 2], (pair[0], pair[1])):
            if sy == 0:
                oa[...] = terms[:, :, :HALF]
            else:
                ra[sy] = terms[:, :, :HALF].astype(BF16)
            if sy == 2:
                ring_send("a", 0, ra.at[2, 0:2])
                ring_send("a", 2, ra.at[2, 2:4])
            elif sy == 1:
                ring_send("a", 1, ra.at[1, 2:4])
            elif sy == 3:
                ring_send("a", 3, ra.at[3, 0:2])
            ob[sy] = terms[0, :, HALF:]
            for sx in range(1, NX):
                rb[sx, sy] = terms[sx, :, HALF:].astype(BF16)
        if i == 0:
            ring_send("b", 2, rb.at[2, 2:4])
            ring_send("b", 1, rb.at[1, 2:4])
        else:
            ring_send("b", 0, rb.at[2, 0:2])
            ring_send("b", 3, rb.at[3, 0:2])

    for colour, mid, sec in (("a", ra, sec_a), ("b", rb, sec_b)):
        rcv = colours[colour][1]
        ring[colour, 0].wait_recv()
        sec[0] = (mid[1, 0:2].astype(F32) + rcv[0].astype(F32)).astype(BF16)
        ring_send(colour, 4, sec.at[0])
        ring[colour, 2].wait_recv()
        sec[1] = (mid[3, 2:4].astype(F32) + rcv[2].astype(F32)).astype(BF16)
        ring_send(colour, 5, sec.at[1])

    second = {}
    for colour, own, s2, r2, send, recv in (("a", oa, s2a, r2a, x2_s, x2_r), ("b", ob, s2b, r2b, y2_s, y2_r)):
        rcv = colours[colour][1]
        ring[colour, 1].wait_recv()
        ring[colour, 3].wait_recv()
        ring[colour, 4].wait_recv()
        ring[colour, 5].wait_recv()
        own[0:2] = own[0:2] + rcv[3].astype(F32) + rcv[4].astype(F32)
        own[2:4] = own[2:4] + rcv[1].astype(F32) + rcv[5].astype(F32)
        for k in (2, 1, 3):
            s2[k] = own[k].astype(BF16)
            to = device(y, xmod(k), z, core) if colour == "a" else device(ymod(k), x, z, core)
            copy = remote(s2.at[k], r2.at[k], send.at[k], recv.at[k], to)
            copy.start()
            sends.append(copy)
            second[colour, k] = copy

    sums = []
    for colour, own, r2 in (("a", oa, r2a), ("b", ob, r2b)):
        total = own[0]
        for k in (1, 3, 2):
            second[colour, k].wait_recv()
            total = total + r2[k].astype(F32)
        sums.append(total)
    total = jnp.concatenate(sums, -1)

    spread_row = iota((NZ * 8, XB), 0)
    spread_of = lax.shift_right_logical(spread_row, 3) * OWN + jnp.bitwise_and(spread_row, 7)
    spread = (spread_of == iota((NZ * 8, XB), 1)) & (jnp.bitwise_and(spread_row, 7) < OWN)
    zs[...] = nn(spread.astype(F32).astype(BF16), total.astype(BF16)).reshape(NZ, 8, D).astype(BF16)
    last = []
    for k in (4, 3, 5, 2, 6, 1, 7):
        copy = remote(zs.at[k], zr.at[k], zz_s.at[k], zz_r.at[k], device(y, x, zmod(k), core))
        copy.start()
        sends.append(copy)
        last.append((k, copy))
    loss_copy.wait_recv()
    loss_ref[...] = (lsend[0:1, 0:1] + lrecv[0:1, 0:1]) * (1.0 / (2 * GROUP))
    final = total[0:OWN]
    for k, copy in reversed(last):
        copy.wait_recv()
        final = final + zr[k].astype(F32)[0:OWN]
    out_ref[...] = final
    for copy in sends:
        copy.wait_send()


def shards(q_hidden, p_hidden, w_up, w_down, pos_index, hard_index):
    vm = pltpu.VMEM
    dma = pltpu.SemaphoreType.DMA
    scratch = [
        pltpu.SMEM((1, 1), jnp.int32), pltpu.SMEM((1, 2), jnp.int32),
        vm((4 * LEN, D), BF16), vm((FF, D), BF16), vm((FF, D), BF16),
        vm((FF // 2, D), BF16), vm((FF // 2, D), BF16), vm((2 * LEN, FF), BF16),
        vm((4 * LEN, D), BF16), vm((4 * LEN, 128), F32), vm((FF // 2, 4 * LEN), F32), vm((4 * LEN, D), BF16),
        vm((NY, 2, 2, NZ, 16, 128), BF16), vm((GROUP * 16, 128), F32), vm((GROUP, D), BF16), vm((GROUP, D), BF16),
        vm((NY, NX, XB, HALF), BF16), vm((NX, NY, XB, HALF), BF16),
        vm((NX, XB, HALF), F32), vm((NY, XB, HALF), F32),
        vm((6, 2, XB, HALF), BF16), vm((6, 2, XB, HALF), BF16),
        vm((2, 2, XB, HALF), BF16), vm((2, 2, XB, HALF), BF16),
        vm((4, XB, HALF), BF16), vm((4, XB, HALF), BF16), vm((4, XB, HALF), BF16), vm((4, XB, HALF), BF16),
        vm((NZ, 8, D), BF16), vm((NZ, 8, D), BF16), vm((8, 128), F32), vm((8, 128), F32),
        dma((4 + 2 * CHUNKS,)), dma((8,)), dma((8,)), dma((8,)), dma((8,)), dma((8,)), dma((8,)), dma((1,)), dma((1,)),
        dma((4,)), dma((4,)), dma((6,)), dma((6,)), dma((6,)), dma((6,)),
        dma((4,)), dma((4,)), dma((4,)), dma((4,)), dma((8,)), dma((8,)),
    ]
    hbm = pl.BlockSpec(memory_space=pltpu.HBM)
    out, loss = pl.pallas_call(
        kernel,
        out_shape=(pltpu.VMEM((OWN, D), F32), pltpu.VMEM((1, 1), F32)),
        in_specs=[hbm, hbm, hbm, hbm, hbm, hbm],
        out_specs=(pl.BlockSpec(memory_space=pltpu.VMEM), pl.BlockSpec(memory_space=pltpu.VMEM)),
        scratch_shapes=scratch,
        compiler_params=pltpu.CompilerParams(
            collective_id=0, has_side_effects=True, vmem_limit_bytes=VMEM_LIMIT
        ),
    )(pos_index, hard_index[0], q_hidden[0, 0], p_hidden[0, 0], w_up, w_down)
    return out, loss[0, 0]


def solution(mesh):
    return jax.shard_map(
        shards,
        mesh=mesh,
        in_specs=(
            P("rep", "dp", None, None),
            P("rep", "dp", None, None),
            P(),
            P(),
            P("rep", "dp"),
            P("rep", "dp", None),
        ),
        out_specs=(P(("dp", "rep"), None), P()),
        check_vma=False,
    )
```

```python
import math

import jax
import jax.numpy as jnp
from jax import lax
from jax.experimental import pallas as pl
from jax.experimental.pallas import tpu as pltpu
from jax.sharding import PartitionSpec as P

MESH = pl.DeviceIdType.MESH
BF16 = jnp.bfloat16
F32 = jnp.float32

NX, NY, NZ = 4, 4, 8
D, FF, LEN = 768, 1536, 128
GROUP = 128
NORM_EPS = 1e-06
HARD_BOOST = 1.5
CHUNKS = 3
CH = FF // CHUNKS
YB = FF // NY
CB = YB // 2
XB = CB // NX
ORDER = (2, 1, 3, 0)
WIDE = D + 128
HALF = D // 2
OWN = XB // NZ
VMEM_LIMIT = 56 * 1024 * 1024


def nt(left, right):
    return lax.dot_general(left, right, (((1,), (1,)), ((), ())), preferred_element_type=F32)


def nn(left, right):
    return lax.dot_general(left, right, (((1,), (0,)), ((), ())), preferred_element_type=F32)


def cdf(v):
    return 0.5 * (1.0 + lax.erf(v * (1.0 / math.sqrt(2.0))))


def iota(shape, dim):
    return lax.broadcasted_iota(jnp.int32, shape, dim)


def kernel(
    pos_hbm, hard_hbm, q_hbm, p_hbm, wup_hbm, wdn_hbm,
    out_ref, loss_ref,
    pos_ref, hard_ref, x_v, wup_v, wdn_v, wupp_v, wdnp_v, normed_v, scale_v, slope_v, along_v,
    tiles, spread_v, gb, gp_v,
    ra, rb, oa, ob, rcv_a, rcv_b, sec_a, sec_b, s2a, s2b, r2a, r2b, zs, zr, lsend, lrecv,
    sem_in, z_s, z_r, g_s, g_r, c_s, c_r, l_s, l_r, core_s, core_r, a_s, a_r, b_s, b_r, x2_s, x2_r, y2_s, y2_r, zz_s, zz_r,
):
    dp = lax.axis_index("dp")
    xh = lax.axis_index("rep")
    core = lax.rem(dp, 2)
    z = lax.rem(lax.div(dp, 2), NZ)
    xl = lax.rem(lax.div(dp, 2 * NZ), 2)
    y = lax.div(dp, 4 * NZ)
    x = xh * 2 + xl

    def device(y_, x_, z_, core_):
        return (((y_ * 2 + lax.rem(x_, 2)) * NZ + z_) * 2 + core_, lax.div(x_, 2))

    def ymod(k):
        return lax.rem(y + k, NY)

    def xmod(k):
        return lax.rem(x + k, NX)

    def zmod(k):
        return lax.rem(z + k, NZ)

    partner = device(y, x, z, 1 - core)

    def plane(dy, dxl):
        xl_ = lax.rem(xl + dxl, 2)
        return ymod(dy), xl_, device(ymod(dy), xh * 2 + xl_, z, core)

    loads = []

    def load(src, dst):
        copy = pltpu.make_async_copy(src, dst, sem_in.at[len(loads)])
        copy.start()
        loads.append(copy)
        return copy

    x_loads = [load(q_hbm, x_v.at[0:LEN]), load(p_hbm, x_v.at[LEN : 2 * LEN])]
    up_loads = [load(wup_hbm.at[rows], wup_v.at[rows]) for rows in (slice(0, CH), slice(CH, FF))]
    dn_load = load(wdn_hbm, wdn_v)
    index_loads = [load(pos_hbm, pos_ref), load(hard_hbm, hard_ref)]

    barrier = pltpu.get_barrier_semaphore()
    peers = [partner]
    peers += [device(y, x, zmod(k), core) for k in range(1, NZ)]
    peers += [plane(dy, dxl)[2] for dy in range(NY) for dxl in range(2) if dy or dxl]
    peers += [device(y, xmod(k), z, core) for k in range(1, NX)]
    for peer in peers:
        pl.semaphore_signal(barrier, inc=1, device_id=peer, device_id_type=MESH)

    for copy in x_loads:
        copy.wait()
    tokens = x_v[: 2 * LEN, :]
    hidden, pre = [], None
    for c in range(CHUNKS):
        if c < 2:
            up_loads[c].wait()
        done, pre = pre, nt(tokens, wup_v[c * CH : (c + 1) * CH, :])
        if c:
            hidden.append((done * cdf(done)).astype(BF16))
    dn_load.wait()
    hidden.append((pre * cdf(pre)).astype(BF16))
    summed = tokens.astype(F32)
    for c in range(CHUNKS):
        summed = summed + nn(hidden[c], wdn_v[c * CH : (c + 1) * CH, :])
    centred = summed - jnp.mean(summed, -1, keepdims=True)
    inv_scale = lax.rsqrt(jnp.mean(centred * centred, -1, keepdims=True) + NORM_EPS)
    normed = centred * inv_scale
    normed_v[: 2 * LEN, :] = normed.astype(BF16)
    embed_q = jnp.sum(normed[:LEN], 0, keepdims=True) * (1.0 / LEN)
    embed_p = jnp.sum(normed[LEN:], 0, keepdims=True) * (1.0 / LEN)

    for copy in index_loads:
        copy.wait()
    row = iota((16, 128), 0)
    lane = iota((16, 128), 1)
    tile = jnp.zeros((16, 128), F32)
    for k in range(6):
        tile = jnp.where(row == k, embed_q[:, k * 128 : (k + 1) * 128], tile)
        tile = jnp.where(row == 6 + k, embed_p[:, k * 128 : (k + 1) * 128], tile)
    named = jnp.where(lane == 0, pos_ref[0, 0], jnp.where(lane == 1, hard_ref[0, 0], hard_ref[0, 1]))
    tile = jnp.where(row == 12, named.astype(F32), tile)
    tiles[z] = tile.astype(BF16)

    pl.semaphore_wait(barrier, len(peers))

    def remote(src, dst, send, recv, to):
        return pltpu.make_async_remote_copy(
            src_ref=src, dst_ref=dst, send_sem=send, recv_sem=recv, device_id=to, device_id_type=MESH
        )

    sends = []
    own_tile = tiles.at[z]
    for k in range(1, NZ):
        copy = remote(own_tile, own_tile, z_s.at[k], z_r.at[k], device(y, x, zmod(k), core))
        copy.start()
        sends.append(copy)

    scale_v[0] = jnp.transpose(jnp.broadcast_to(inv_scale, (2 * LEN, 128)))[0:8]
    shared = []
    for k, (own, theirs) in enumerate((
        (x_v.at[: 2 * LEN], x_v.at[2 * LEN :]),
        (normed_v.at[: 2 * LEN], normed_v.at[2 * LEN :]),
        (scale_v.at[0], scale_v.at[1]),
    )):
        copy = remote(own, theirs, core_s.at[k], core_r.at[k], partner)
        copy.start()
        shared.append(copy)
        sends.append(copy)

    out_row = iota((CB, YB), 0)
    in_row = iota((CB, YB), 1)
    unit = lax.shift_right_logical(out_row * 10923, 16)
    inner = out_row - unit * 6
    slot_z = jnp.bitwise_and(unit, 7)
    slot_x = lax.shift_right_logical(unit, 3)
    to_z = jnp.bitwise_and(slot_z + z, 7)
    to_x = jnp.bitwise_and(slot_x + x, 3)
    to_xh = lax.shift_right_logical(to_x, 1)
    to_xl = jnp.bitwise_and(to_x, 1)
    source = (((to_xl * NZ + to_z) * 2 + core) * 2 + to_xh) * 6 + inner
    reorder = (source == in_row).astype(F32).astype(BF16)
    for i, sy in enumerate(ORDER):
        rows = pl.ds(pl.multiple_of(ymod(sy) * YB, YB), YB)
        wdnp_v[i * CB : (i + 1) * CB, :] = nn(reorder, wdn_v[rows, :]).astype(BF16)
        wupp_v[i * CB : (i + 1) * CB, :] = nn(reorder, wup_v[rows, :]).astype(BF16)

    for k in range(1, NZ):
        landed = tiles.at[zmod(NZ - k)]
        remote(landed, landed, z_s.at[k], z_r.at[k], device(y, x, zmod(k), core)).wait_recv()
    spread_v[...] = tiles[...].reshape(NZ * 16, 128).astype(F32)
    own_line = gb.at[y, xl, core]
    for k in range(7):
        upper = spread_v[pl.ds(12 if k == 6 else k, NZ, stride=16), :]
        lower = spread_v[pl.ds(12 if k == 6 else 6 + k, NZ, stride=16), :]
        own_line[:, k * 128 : (k + 1) * 128] = jnp.concatenate([upper, lower], 0).astype(BF16)
    copy = remote(own_line, own_line, c_s.at[0], c_r.at[0], partner)
    copy.start()
    sends.append(copy)
    offsets = [(0, 1), (1, 0), (3, 0), (1, 1), (3, 1), (2, 0), (2, 1)]
    for dy, dxl in offsets:
        copy = remote(own_line, own_line, g_s.at[dy * 2 + dxl], g_r.at[dy * 2 + dxl], plane(dy, dxl)[2])
        copy.start()
        sends.append(copy)

    for copy in shared:
        copy.wait_recv()
    both = x_v[...]
    scale = jnp.concatenate([scale_v[0, 0:1, :], scale_v[1, 0:1, :]], 1)
    for i in range(2):
        block = slice(i * YB, (i + 1) * YB)
        pre = nt(wupp_v[block, :], both)
        slope = (cdf(pre) + pre * jnp.exp(-0.5 * pre * pre) * (1.0 / math.sqrt(2.0 * math.pi))) * scale
        slope_v[block, :] = slope
        along_v[block, :] = slope * nt(wdnp_v[block, :], normed_v[...])

    for dy, dxl in offsets:
        y_, xl_, _ = plane(NY - dy, dxl)
        landed = gb.at[y_, xl_, core]
        remote(landed, landed, g_s.at[dy * 2 + dxl], g_r.at[dy * 2 + dxl], partner).wait_recv()
        copy = remote(landed, landed, c_s.at[dy * 2 + dxl], c_r.at[dy * 2 + dxl], partner)
        copy.start()
        sends.append(copy)
    for dy, dxl in [(0, 0)] + offsets:
        y_, xl_, _ = plane(NY - dy, dxl)
        landed = gb.at[y_, xl_, 1 - core]
        remote(landed, landed, c_s.at[dy * 2 + dxl], c_r.at[dy * 2 + dxl], partner).wait_recv()

    everyone = gb[...].reshape(2 * GROUP, WIDE)
    sequences = everyone[:, :D]
    names = everyone[:, D:].astype(F32)
    scores = nt(sequences, sequences)
    place = iota((2 * GROUP, 2 * GROUP), 1)
    line = lax.shift_right_logical(place, 4)
    group_index = (
        lax.shift_right_logical(line, 1) * 16 + jnp.bitwise_and(place, 7) * 2 + jnp.bitwise_and(line, 1)
    ).astype(F32)
    is_passage = jnp.bitwise_and(place, 8) == 8
    target = (names[:, 0:1] == group_index) & is_passage
    hard = (names[:, 1:2] == group_index) | (names[:, 2:3] == group_index)
    logits = scores + jnp.where(hard, HARD_BOOST, 0.0)
    row_max = jnp.max(jnp.where(is_passage, logits, -jnp.inf), -1, keepdims=True)
    powers = jnp.where(is_passage, jnp.exp(logits - row_max), 0.0)
    power_sum = jnp.sum(powers, -1, keepdims=True)
    log_total = row_max + jnp.log(power_sum)
    picked = jnp.sum(jnp.where(target, logits, 0.0), -1, keepdims=True)
    row_is_query = jnp.bitwise_and(iota((2 * GROUP, 2 * GROUP), 0), 8) == 0
    loss_sum = jnp.sum(jnp.where(row_is_query[:, 0:1], log_total - picked, 0.0), 0, keepdims=True)
    lsend[...] = jnp.broadcast_to(loss_sum, (8, 128))
    softmax = jnp.where(is_passage, jnp.exp(logits - log_total), 0.0)
    weights = jnp.where(row_is_query, softmax - jnp.where(target, 1.0, 0.0), 0.0).astype(BF16)
    pick_row = iota((16, 2 * GROUP), 0)
    other_core = jnp.bitwise_and(lax.shift_right_logical(pick_row, 1), 1)
    pick_core = other_core + core - 2 * other_core * core
    pick_part = jnp.bitwise_and(pick_row, 1)
    mine = iota((16, 2 * GROUP), 1) == (((y * 2 + xl) * 2 + pick_core) * 2 + pick_part) * NZ + z
    own_row = nn((mine & (pick_part == 0)).astype(F32).astype(BF16), weights).astype(BF16)
    own_col = nt((mine & (pick_part == 1)).astype(F32).astype(BF16), weights).astype(BF16)
    grad = nn(own_row + own_col, sequences) * (1.0 / LEN)
    parts = (grad - jnp.mean(grad, -1, keepdims=True)).astype(BF16)

    other = device(y, xmod(2), z, core)
    loss_copy = remote(lsend, lrecv, l_s.at[0], l_r.at[0], other)
    loss_copy.start()
    sends.append(loss_copy)

    along_all = nt(parts, normed_v[...]) * (1.0 / D)
    across_all = nt(wdnp_v[...], parts)
    spans = [slice(k * LEN, (k + 1) * LEN) for k in range(4)]
    along = [along_all[k : k + 1, span] for k, span in enumerate(spans)]
    for i in range(4):
        block = slice(i * CB, (i + 1) * CB)
        for k, span in enumerate(spans):
            late = across_all[block, k : k + 1] * slope_v[block, span] - along[k] * along_v[block, span]
            gp_v[i, :, :, span] = late.astype(BF16).reshape(NX, XB, LEN)

    y_up, y_dn = device(ymod(1), x, z, core), device(ymod(3), x, z, core)
    x_up, x_dn = device(y, xmod(1), z, core), device(y, xmod(3), z, core)
    colours = {"a": (ra, rcv_a, a_s, a_r, y_up, y_dn), "b": (rb, rcv_b, b_s, b_r, x_up, x_dn)}
    ring = {}

    def ring_send(colour, index, src, rcv, up):
        _, _, send, recv, to_up, to_down = colours[colour]
        copy = remote(src, rcv, send.at[index], recv.at[index], to_up if up else to_down)
        copy.start()
        sends.append(copy)
        ring[colour, index] = copy

    def relay(colour, piece):
        mid, rcv = colours[colour][:2]
        ring_send(colour, piece, mid.at[2, piece], rcv.at[piece], piece < 2)

    def direct(colour, up):
        mid, rcv = colours[colour][:2]
        if up:
            ring_send(colour, 8, mid.at[1, 2:4], rcv.at[10:12], True)
        else:
            ring_send(colour, 9, mid.at[3, 0:2], rcv.at[8:10], False)

    def terms(rows, right):
        cols = slice(HALF, D) if right else slice(0, HALF)
        return nn(rows.reshape(-1, 4 * LEN), x_v[:, cols]).reshape(-1, 4, XB, HALF)

    ra[2] = terms(gp_v[0], False)[0].astype(BF16)
    for piece in (2, 1, 3, 0):
        relay("a", piece)
    far = terms(gp_v[:, 2], True)[0].astype(BF16)
    for i in range(4):
        rb[2, ORDER[i]] = far[i]
    for piece in (2, 1, 3, 0):
        relay("b", piece)
    near = terms(gp_v[1:3], False).astype(BF16)
    ra[1] = near[0]
    ra[3] = near[1]
    direct("a", True)
    direct("a", False)
    near = terms(jnp.concatenate([gp_v[:, 1], gp_v[:, 3]], 0), True).astype(BF16)
    for i in range(4):
        rb[1, ORDER[i]] = near[0, i]
        rb[3, ORDER[i]] = near[1, i]
    direct("b", True)
    direct("b", False)
    oa[...] = terms(gp_v[3], False)[0]
    home = terms(gp_v[:, 0], True)[0]
    for i in range(4):
        ob[ORDER[i]] = home[i]

    for colour, piece in (("a", 2), ("a", 1), ("b", 2), ("b", 1), ("a", 3), ("a", 0), ("b", 3), ("b", 0)):
        mid, rcv = colours[colour][:2]
        sec = sec_a if colour == "a" else sec_b
        ring[colour, piece].wait_recv()
        sec[piece] = (mid[1 if piece < 2 else 3, piece].astype(F32) + rcv[piece].astype(F32)).astype(BF16)
        ring_send(colour, 4 + piece, sec.at[piece], rcv.at[4 + piece], piece < 2)

    second = {}
    seconds = {"a": (oa, s2a, r2a, x2_s, x2_r), "b": (ob, s2b, r2b, y2_s, y2_r)}
    for piece in (2, 1, 3, 0):
        for colour in ("a", "b"):
            own, s2, r2, send, recv = seconds[colour]
            rcv = colours[colour][1]
            if piece in (1, 2):
                ring[colour, 9 if piece < 2 else 8].wait_recv()
            ring[colour, 4 + piece].wait_recv()
            total = own[piece] + rcv[8 + piece].astype(F32) + rcv[4 + piece].astype(F32)
            if piece == 0:
                own[0] = total
                continue
            s2[piece] = total.astype(BF16)
            to = device(y, xmod(piece), z, core) if colour == "a" else device(ymod(piece), x, z, core)
            copy = remote(s2.at[piece], r2.at[piece], send.at[piece], recv.at[piece], to)
            copy.start()
            sends.append(copy)
            second[colour, piece] = copy

    sums = []
    for colour, own, r2 in (("a", oa, r2a), ("b", ob, r2b)):
        total = own[0]
        for k in (1, 3, 2):
            second[colour, k].wait_recv()
            total = total + r2[k].astype(F32)
        sums.append(total)
    total = jnp.concatenate(sums, -1)

    spread_row = iota((NZ * 8, XB), 0)
    spread_of = lax.shift_right_logical(spread_row, 3) * OWN + jnp.bitwise_and(spread_row, 7)
    spread = (spread_of == iota((NZ * 8, XB), 1)) & (jnp.bitwise_and(spread_row, 7) < OWN)
    zs[...] = nn(spread.astype(F32).astype(BF16), total.astype(BF16)).reshape(NZ, 8, D).astype(BF16)
    last = []
    for k in (4, 3, 5, 2, 6, 1, 7):
        copy = remote(zs.at[k], zr.at[k], zz_s.at[k], zz_r.at[k], device(y, x, zmod(k), core))
        copy.start()
        sends.append(copy)
        last.append((k, copy))
    loss_copy.wait_recv()
    loss_ref[...] = (lsend[0:1, 0:1] + lrecv[0:1, 0:1]) * (1.0 / (2 * GROUP))
    final = total[0:OWN]
    for k, copy in reversed(last):
        copy.wait_recv()
        final = final + zr[k].astype(F32)[0:OWN]
    out_ref[...] = final
    for copy in sends:
        copy.wait_send()


def shards(q_hidden, p_hidden, w_up, w_down, pos_index, hard_index):
    vm = pltpu.VMEM
    dma = pltpu.SemaphoreType.DMA
    scratch = [
        pltpu.SMEM((1, 1), jnp.int32), pltpu.SMEM((1, 2), jnp.int32),
        vm((4 * LEN, D), BF16), vm((FF, D), BF16), vm((FF, D), BF16),
        vm((FF // 2, D), BF16), vm((FF // 2, D), BF16),
        vm((4 * LEN, D), BF16), vm((2, 8, 2 * LEN), F32), vm((FF // 2, 4 * LEN), F32), vm((FF // 2, 4 * LEN), F32),
        vm((NZ, 16, 128), BF16), vm((NZ * 16, 128), F32), vm((NY, 2, 2, 16, WIDE), BF16),
        vm((4, NX, XB, 4 * LEN), BF16),
        vm((NY, NX, XB, HALF), BF16), vm((NX, NY, XB, HALF), BF16),
        vm((NX, XB, HALF), F32), vm((NY, XB, HALF), F32),
        vm((12, XB, HALF), BF16), vm((12, XB, HALF), BF16),
        vm((4, XB, HALF), BF16), vm((4, XB, HALF), BF16),
        vm((4, XB, HALF), BF16), vm((4, XB, HALF), BF16), vm((4, XB, HALF), BF16), vm((4, XB, HALF), BF16),
        vm((NZ, 8, D), BF16), vm((NZ, 8, D), BF16), vm((8, 128), F32), vm((8, 128), F32),
        dma((7,)), dma((8,)), dma((8,)), dma((8,)), dma((8,)), dma((8,)), dma((8,)), dma((1,)), dma((1,)),
        dma((4,)), dma((4,)), dma((10,)), dma((10,)), dma((10,)), dma((10,)),
        dma((4,)), dma((4,)), dma((4,)), dma((4,)), dma((8,)), dma((8,)),
    ]
    hbm = pl.BlockSpec(memory_space=pltpu.HBM)
    out, loss = pl.pallas_call(
        kernel,
        out_shape=(pltpu.VMEM((OWN, D), F32), pltpu.VMEM((1, 1), F32)),
        in_specs=[hbm, hbm, hbm, hbm, hbm, hbm],
        out_specs=(pl.BlockSpec(memory_space=pltpu.VMEM), pl.BlockSpec(memory_space=pltpu.VMEM)),
        scratch_shapes=scratch,
        compiler_params=pltpu.CompilerParams(
            collective_id=0, has_side_effects=True, vmem_limit_bytes=VMEM_LIMIT
        ),
    )(pos_index, hard_index[0], q_hidden[0, 0], p_hidden[0, 0], w_up, w_down)
    return out, loss[0, 0]


def solution(mesh):
    return jax.shard_map(
        shards,
        mesh=mesh,
        in_specs=(
            P("rep", "dp", None, None),
            P("rep", "dp", None, None),
            P(),
            P(),
            P("rep", "dp"),
            P("rep", "dp", None),
        ),
        out_specs=(P(("dp", "rep"), None), P()),
        check_vma=False,
    )
```
